32 devices in a mesh: dp: 32 (over z, y, x, core), mp: 1.
Axes of the slice: x: 2, y: 2, z: 4, core: 2. Of those that a mesh axis runs over, the one named last changes fastest.
Arguments:
- gradients: bfloat16 [32, 512, 6144], P('dp', None, 'mp'), may hold values from -48 to 48
- weights: bfloat16 [512, 6144], P(None, 'mp'), may hold values from -3 to 3
- master: float32 [512, 6144], P('dp', 'mp'), may hold values from -6 to 6
- moment_one: float32 [512, 6144], P('dp', 'mp'), may hold values from -6 to 6
- moment_two: float32 [512, 6144], P('dp', 'mp'), may hold values from 0.25 to 4
- group_ids: int32 [512], replicated, may hold values from 0 to 15, never falling along the last dimension, each value on 1 to 64 neighbouring positions
Outputs:
- new_weights: bfloat16 [512, 6144], P(None, 'mp')
- new_master: float32 [512, 6144], P('dp', 'mp')
- new_first: float32 [512, 6144], P('dp', 'mp')
- new_second: float32 [512, 6144], P('dp', 'mp')
The draws below stay inside these ranges and needn't reach their ends.
Inputs may be any that keep to these rules, and one draw needn't show every extreme that they name: `group_ids`: group numbers never fall along the rows; each group has 1 to 64 rows and every group is present.
All inputs are finite; a program needn't handle non-finite values.
Results may differ from the reference program's by a relative error of at most 0.001.
The reference program's roundings to bfloat16 on the way count: a program that leaves them out, or rounds other values in their place, can miss the bound.
Values may be sent and summed in bfloat16 or wider, within the bound.
No kernel may reach another device: no remote copies, remote signals or barrier semaphores. Data moves between devices by JAX's collectives and lax.ppermute only.
A program may use at most 64 MiB of HBM per device.

```python
import math
import jax
import jax.numpy as jnp
import numpy as np
from jax import lax

D = 6144
MOST = 64
ROWS_ALL = 512
GROUPS = 16
N_DP = 32


def raised(drawn, own_key, source, target, shards_of, factor):
    def block_of(dim):
        return (jnp.arange(drawn.shape[dim]) // (drawn.shape[dim] // shards_of)).reshape((-1,) + (1,) * (drawn.ndim - 1 - dim))

    first = jax.random.permutation(own_key, shards_of)[block_of(target)]
    other_side = (block_of(target) + shards_of // 2) % shards_of
    return jnp.where((block_of(source) == first) | (block_of(source) == other_side), factor * drawn, drawn)


def level_of(rng, extent, split, low, top_value):
    level = 1.0
    for axis_at, shards_of in split:
        draws = jax.random.uniform(jax.random.fold_in(jax.random.fold_in(rng, 6), axis_at), (shards_of,), jnp.float32, low / len(split), top_value / len(split))
        level = level * jnp.repeat(jnp.exp(draws), extent[axis_at] // shards_of).reshape((-1,) + (1,) * (len(extent) - 1 - axis_at))
    return level


def length_profile(amount, total, limit, slope):
    portions = [(1 << 20) // math.isqrt(grade ** slope) + 1 for grade in range(2, amount + 1)]
    rest, holding = total - limit - (amount - 1), [1] * (amount - 1)
    while rest > 0:
        candidates = [i for i in range(amount - 1) if holding[i] < limit]
        pool, budget = sum([portions[i] for i in candidates]), rest
        for i in candidates:
            more = min(limit - holding[i], max(1, budget * portions[i] // pool), rest)
            holding[i] = holding[i] + more
            rest = rest - more
    return np.array([limit] + holding)


def uneven(rng, number_of, total, most, lean):
    if number_of == 2:
        one = jax.random.randint(rng, (), max(1, total - most), min(most, total - 1) + 1)
        return jnp.stack([one, total - one])
    sizes = jnp.asarray(length_profile(number_of, total, most, lean), jnp.int32)
    pairs = (number_of - 1) // 2
    giver, sink = sizes[1:1 + 2 * pairs:2], sizes[2:2 + 2 * pairs:2]
    slack = jnp.minimum(giver - 1, most - sink)
    moved = jax.random.randint(jax.random.fold_in(rng, 1), (pairs,), 0, 1 << 20) % (slack + 1)
    sizes = sizes.at[1:1 + 2 * pairs:2].set(giver - moved).at[2:2 + 2 * pairs:2].set(sink + moved)
    return sizes[jax.random.permutation(jax.random.fold_in(rng, 2), number_of)]


def normal_values(stream_key, dims, deviation, most, shards=(), held_as=jnp.bfloat16):
    entries = deviation * jax.random.normal(stream_key, dims, jnp.float32)
    if shards:
        entries = entries * level_of(stream_key, dims, shards, -0.22, 0.18)
    return jnp.clip(entries, -most, most).astype(held_as)


def gaussian_with(stream_key, dims, scale, limit, pieces, heavy, kind=jnp.bfloat16):
    entries = scale * jax.random.normal(stream_key, dims, jnp.float32)
    if pieces:
        entries = entries * level_of(stream_key, dims, pieces, -0.22, 0.18)
    return jnp.clip(raised(entries, jax.random.fold_in(stream_key, 3), *heavy), -limit, limit).astype(kind)


def setup_inputs(seed: int = 0) -> dict:
    key_list = jax.random.split(jax.random.key(seed), 7)
    return {
        "gradients": gaussian_with(key_list[0], (N_DP, ROWS_ALL, D), 8.0, 48.0, ((0, 32),), (0, 1, 32, 2.75)),
        "weights": normal_values(key_list[1], (ROWS_ALL, D), 0.5, 3.0),
        "master": normal_values(key_list[2], (ROWS_ALL, D), 1.0, 6.0, ((0, 32),), jnp.float32),
        "moment_one": normal_values(key_list[3], (ROWS_ALL, D), 1.0, 6.0, ((0, 32),), jnp.float32),
        "moment_two": jnp.clip(jnp.exp(math.log(4.0) - 2.7725887 * jax.random.uniform(key_list[4], (ROWS_ALL, D), jnp.float32) ** level_of(key_list[4], (ROWS_ALL, D), ((0, 32),), -0.2, 0.2)), 0.25, 4.0),
        "group_ids": jnp.searchsorted(jnp.cumsum(uneven(key_list[5], GROUPS, ROWS_ALL, MOST, 0)), jnp.arange(ROWS_ALL), side="right").astype(jnp.int32),
    }


beta_one = 0.9
beta_two = 0.999
adam_eps = 1e-06
weight_decay = 0.01
learn_rate = 0.04
step_count = 100

def reference(gradients, weights, master, moment_one, moment_two, group_ids):
    grad_mean = lax.optimization_barrier(jnp.sum(gradients, axis=0, dtype=jnp.float32)) / N_DP
    new_first = beta_one * moment_one + (1.0 - beta_one) * grad_mean
    new_second = beta_two * moment_two + (1.0 - beta_two) * grad_mean * grad_mean
    correct_one = 1.0 - beta_one ** step_count
    correct_two = 1.0 - beta_two ** step_count
    update = new_first / correct_one / (jnp.sqrt(new_second / correct_two) + adam_eps) + weight_decay * master
    member = (group_ids[:, None] == jnp.arange(GROUPS, dtype=jnp.int32)[None, :]).astype(jnp.float32)
    weight_sq = jnp.dot(lax.optimization_barrier(jnp.sum(master * master, axis=1)), member, precision=lax.Precision.HIGHEST)
    update_sq = jnp.dot(lax.optimization_barrier(jnp.sum(update * update, axis=1)), member, precision=lax.Precision.HIGHEST)
    trust_ratio = jnp.sqrt(weight_sq / (update_sq + 1e-06))
    row_ratio = jnp.dot(member, trust_ratio, precision=lax.Precision.HIGHEST)
    step_size = learn_rate * row_ratio[:, None] * update
    new_master = master - step_size
    delta_bf = lax.optimization_barrier((-step_size).astype(jnp.bfloat16))
    new_weights = (weights.astype(jnp.float32) + delta_bf.astype(jnp.float32)).astype(jnp.bfloat16)
    return (new_weights, new_master, new_first, new_second)
```

```python
import jax
import jax.numpy as jnp
from jax import lax
from jax.sharding import PartitionSpec as P

beta_one = 0.9
beta_two = 0.999
adam_eps = 1e-06
weight_decay = 0.01
learn_rate = 0.04
step_count = 100


def swap(value, mask):
    replicas = lax.axis_size("dp")
    return lax.ppermute(value, "dp", [(i, i ^ mask) for i in range(replicas)])


def pick(value, bits, bit, side):
    at = bits.index(bit)
    rest = bits[:at] + bits[at + 1 :]
    halves = value.reshape((1 << at, 2, 1 << (len(rest) - at)) + value.shape[1:])
    half = lax.dynamic_index_in_dim(halves, side, 1, keepdims=False)
    return half.reshape((1 << len(rest),) + value.shape[1:]), rest


def join(mine, theirs, bits, bit, side):
    at = len([b for b in bits if b > bit])
    shape = (1 << at, 1 << (len(bits) - at)) + mine.shape[1:]
    mine, theirs = mine.reshape(shape), theirs.reshape(shape)
    first = jnp.where(side == 0, mine, theirs)
    second = jnp.where(side == 0, theirs, mine)
    both = jnp.stack([first, second], axis=1)
    return both.reshape((2 << len(bits),) + mine.shape[2:]), bits[:at] + [bit] + bits[at:]


def total(terms):
    out = terms[0].astype(jnp.float32)
    for term in terms[1:]:
        out = out + term.astype(jnp.float32)
    return out


def scatter_sum(grad, bits, order, side):
    a, b = order[:2]

    def quarter(fa, fb):
        part, rest = pick(grad, bits, a, side[a] ^ fa)
        return pick(part, rest, b, side[b] ^ fb)

    terms = [swap(quarter(fa, fb)[0], (fa << a) | (fb << b)) for fa, fb in ((0, 1), (1, 1), (1, 0))]
    own, bits = quarter(0, 0)
    terms = [own] + terms
    for bit in order[2:]:
        sent = total([pick(t, bits, bit, 1 - side[bit])[0] for t in terms])
        got = swap(sent, 1 << bit)
        kept = [pick(t, bits, bit, side[bit]) for t in terms]
        bits = kept[0][1]
        terms = [k[0] for k in kept] + [got]
    return total(terms)[0]


def on_device(gradients, weights, master, moment_one, moment_two, group_ids):
    owned_rows, width = master.shape
    rows_all = weights.shape[0]
    groups = rows_all // 32
    replicas = lax.axis_size("dp")
    count = replicas.bit_length() - 1
    half = owned_rows // 2
    my_index = lax.axis_index("dp")
    side = [(my_index >> k) & 1 for k in range(count)]
    first_own = my_index * owned_rows
    my_groups = lax.dynamic_slice_in_dim(group_ids, first_own, owned_rows, 0)
    member = (my_groups[:, None] == jnp.arange(groups, dtype=jnp.int32)[None, :]).astype(
        jnp.float32
    )
    weight_rows = jnp.dot(jnp.sum(master * master, axis=1), member, precision=lax.Precision.HIGHEST)

    down = list(range(count))[::-1]
    orders = ([1, 0] + list(range(2, count)), [2, 0, 1] + list(range(3, count))[::-1])
    grad = gradients[0].reshape(replicas, 2, half, width)
    summed = jnp.concatenate(
        [scatter_sum(grad[:, color], down, orders[color], side) for color in range(2)], axis=0
    )
    grad_mean = summed / replicas
    new_first = beta_one * moment_one + (1.0 - beta_one) * grad_mean
    new_second = beta_two * moment_two + (1.0 - beta_two) * grad_mean * grad_mean
    correct_one = 1.0 - beta_one**step_count
    correct_two = 1.0 - beta_two**step_count
    update = (
        new_first / correct_one / (jnp.sqrt(new_second / correct_two) + adam_eps)
        + weight_decay * master
    )
    update_rows = jnp.dot(jnp.sum(update * update, axis=1), member, precision=lax.Precision.HIGHEST)
    squares = jnp.stack([weight_rows, update_rows])
    if lax.axis_size("mp") > 1:
        squares = lax.psum(squares, "mp")
    low = 0
    while low < count:
        span = min(3 if low == 0 else 2, count - low)
        parts = [swap(squares, offset << low) for offset in range(1, 1 << span)]
        squares = total([squares] + parts)
        low += span
    weight_sq, update_sq = squares[0], squares[1]
    trust_ratio = jnp.sqrt(weight_sq / (update_sq + 1e-06))
    row_ratio = jnp.dot(member, trust_ratio, precision=lax.Precision.HIGHEST)
    step_size = learn_rate * row_ratio[:, None] * update
    new_master = master - step_size
    delta_bf = (-step_size).astype(jnp.bfloat16)

    shape = (2,) * count + (2, half, width)
    old = weights.reshape(shape)
    new = old

    def place(new, piece, bits, fixed, color):
        start = [fixed.get(b, 0) for b in down] + [color, 0, 0]
        sizes = [1 if b in fixed else 2 for b in down] + [1, half, width]
        before = lax.dynamic_slice(old, start, sizes)
        after = before.astype(jnp.float32) + piece.reshape(sizes).astype(jnp.float32)
        return lax.dynamic_update_slice(new, after.astype(jnp.bfloat16), start)

    for color in range(2):
        last, _, *middle = orders[color]
        piece, bits = delta_bf[color * half : (color + 1) * half][None], []
        for bit in middle[::-1]:
            piece, bits = join(piece, swap(piece, 1 << bit), bits, bit, side[bit])
        far = swap(piece, 1 << last)
        near_core = swap(piece, 1)
        far_core = swap(far, 1)
        for part, fl, fc in ((piece, 0, 0), (near_core, 0, 1), (far, 1, 0), (far_core, 1, 1)):
            new = place(new, part, bits, {last: side[last] ^ fl, 0: side[0] ^ fc}, color)
    return (new.reshape(rows_all, width), new_master, new_first, new_second)


def solution(mesh):
    placed = (P("dp", None, "mp"), P(None, "mp"), P("dp", "mp"), P("dp", "mp"), P("dp", "mp"), P())
    return jax.shard_map(
        on_device,
        mesh=mesh,
        in_specs=placed,
        out_specs=(P(None, "mp"), P("dp", "mp"), P("dp", "mp"), P("dp", "mp")),
        check_vma=False,
    )
```

```python
import jax
import jax.numpy as jnp
from jax import lax
from jax.sharding import PartitionSpec as P

beta_one = 0.9
beta_two = 0.999
adam_eps = 1e-06
weight_decay = 0.01
learn_rate = 0.04
step_count = 100


def swap(value, mask):
    replicas = lax.axis_size("dp")
    return lax.ppermute(value, "dp", [(i, i ^ mask) for i in range(replicas)])


def pick(value, bits, bit, side):
    at = bits.index(bit)
    rest = bits[:at] + bits[at + 1 :]
    halves = value.reshape((1 << at, 2, 1 << (len(rest) - at)) + value.shape[1:])
    half = lax.dynamic_index_in_dim(halves, side, 1, keepdims=False)
    return half.reshape((1 << len(rest),) + value.shape[1:]), rest


def join(mine, theirs, bits, bit, side):
    at = len([b for b in bits if b > bit])
    shape = (1 << at, 1 << (len(bits) - at)) + mine.shape[1:]
    mine, theirs = mine.reshape(shape), theirs.reshape(shape)
    first = jnp.where(side == 0, mine, theirs)
    second = jnp.where(side == 0, theirs, mine)
    both = jnp.stack([first, second], axis=1)
    return both.reshape((2 << len(bits),) + mine.shape[2:]), bits[:at] + [bit] + bits[at:]


def total(terms):
    out = terms[0].astype(jnp.float32)
    for term in terms[1:]:
        out = out + term.astype(jnp.float32)
    return out


def after(values, token):
    return list(lax.optimization_barrier(tuple(values) + (token,)))[:-1]


def scatter_sums(grad, colors, down, side):
    held = []
    for order, r0, r1, c0, c1 in colors:
        a, b = order[:2]
        rest = [k for k in down if k not in (a, b)]

        def quarter(fa, fb):
            at = {a: side[a] ^ fa, b: side[b] ^ fb}
            start = [at.get(k, 0) for k in down] + [r0, c0]
            sizes = [1 if k in at else 2 for k in down] + [r1 - r0, c1 - c0]
            return lax.dynamic_slice(grad, start, sizes).reshape((1 << len(rest), r1 - r0, c1 - c0))

        got = [swap(quarter(fa, fb), (fa << a) | (fb << b)) for fa, fb in ((1, 1), (1, 0), (0, 1))]
        held.append((quarter(0, 0), got, rest))
    token = None
    for step in range(2, len(down)):
        for at, (order, *_) in enumerate(colors):
            bit = order[step]
            own, got, bits = held[at]
            if token is not None:
                got = after(got, token)
            sent = total([pick(t, bits, bit, 1 - side[bit])[0] for t in [own] + got])
            token = sent
            new = swap(sent, 1 << bit)
            own, rest = pick(own, bits, bit, side[bit])
            held[at] = (own, [pick(t, bits, bit, side[bit])[0] for t in got] + [new], rest)
    return [total([own] + got)[0] for own, got, _ in held]


def on_device(gradients, weights, master, moment_one, moment_two, group_ids):
    owned_rows, width = master.shape
    rows_all = weights.shape[0]
    groups = rows_all // 32
    replicas = lax.axis_size("dp")
    count = replicas.bit_length() - 1
    half = owned_rows // 2
    my_index = lax.axis_index("dp")
    side = [(my_index >> k) & 1 for k in range(count)]
    first_own = my_index * owned_rows
    my_groups = lax.dynamic_slice_in_dim(group_ids, first_own, owned_rows, 0)
    member = (my_groups[:, None] == jnp.arange(groups, dtype=jnp.int32)[None, :]).astype(
        jnp.float32
    )
    weight_rows = jnp.dot(jnp.sum(master * master, axis=1), member, precision=lax.Precision.HIGHEST)

    down = list(range(count))[::-1]
    third = width // 3 // 128 * 128
    colors = (
        ([1, 0, 2] + list(range(3, count)), 0, half, third, width),
        ([2, 0, 1] + list(range(3, count)), half, owned_rows, third, width),
        ([3, 0] + list(range(4, count)) + [1, 2], 0, owned_rows, 0, third),
    )
    grad = gradients[0].reshape((2,) * count + (owned_rows, width))
    sums = scatter_sums(grad, colors, down, side)
    summed = jnp.concatenate([sums[2], jnp.concatenate(sums[:2], axis=0)], axis=1)
    grad_mean = summed / replicas
    new_first = beta_one * moment_one + (1.0 - beta_one) * grad_mean
    new_second = beta_two * moment_two + (1.0 - beta_two) * grad_mean * grad_mean
    correct_one = 1.0 - beta_one**step_count
    correct_two = 1.0 - beta_two**step_count
    update = (
        new_first / correct_one / (jnp.sqrt(new_second / correct_two) + adam_eps)
        + weight_decay * master
    )
    update_rows = jnp.dot(jnp.sum(update * update, axis=1), member, precision=lax.Precision.HIGHEST)

    early = [(update[r0:r1, c0:c1][None], []) for _, r0, r1, c0, c1 in colors]

    def widen(step):
        for at, (order, *_) in enumerate(colors):
            if step < len(order) - 3:
                (piece, bits), bit = early[at], order[-1 - step]
                early[at] = join(piece, swap(piece, 1 << bit), bits, bit, side[bit])
        return early[-1][0]

    squares = jnp.stack([weight_rows, update_rows])
    if lax.axis_size("mp") > 1:
        squares = lax.psum(squares, "mp")
    low, step = 0, 0
    while low < count:
        span = min(2, count - low)
        token = early[-1][0]
        widen(step)
        step += 1
        if low:
            squares, = after([squares], token)
        parts = [squares] + [swap(squares, offset << low) for offset in range(1, 1 << span)]
        while len(parts) > 1:
            parts = [parts[i] + parts[i + 1] for i in range(0, len(parts), 2)]
        squares = parts[0]
        low += span
    while step < count - 3:
        widen(step)
        step += 1
    trust_ratio = jnp.sqrt(squares[0] / (squares[1] + 1e-06))
    all_member = group_ids[:, None] == jnp.arange(groups, dtype=jnp.int32)[None, :]
    row_scale = learn_rate * jnp.sum(jnp.where(all_member, trust_ratio[None, :], 0.0), axis=1)
    own_scale = lax.dynamic_slice_in_dim(row_scale, first_own, owned_rows, 0)
    new_master = master - own_scale[:, None] * update

    row_scale = row_scale.reshape(replicas, owned_rows)
    old = weights.reshape((2,) * count + (owned_rows, width))
    new = old
    for (order, r0, r1, c0, c1), (piece, bits) in zip(colors, early):
        scale, left = row_scale[:, r0:r1], down
        for bit in [b for b in down if b not in bits]:
            scale, left = pick(scale, left, bit, side[bit])
        piece = (-(scale[:, :, None] * piece)).astype(jnp.bfloat16)
        piece, bits = join(piece, swap(piece, 1 << order[2]), bits, order[2], side[order[2]])
        last = order[0]
        far = swap(piece, 1 << last)
        near_core = swap(piece, 1)
        far_core = swap(far, 1)
        for part, fl, fc in ((piece, 0, 0), (near_core, 0, 1), (far, 1, 0), (far_core, 1, 1)):
            fixed = {last: side[last] ^ fl, 0: side[0] ^ fc}
            start = [fixed.get(b, 0) for b in down] + [r0, c0]
            sizes = [1 if b in fixed else 2 for b in down] + [r1 - r0, c1 - c0]
            before = lax.dynamic_slice(old, start, sizes).astype(jnp.float32)
            moved = before + part.reshape(sizes).astype(jnp.float32)
            new = lax.dynamic_update_slice(new, moved.astype(jnp.bfloat16), start)
    return (new.reshape(rows_all, width), new_master, new_first, new_second)


def solution(mesh):
    placed = (P("dp", None, "mp"), P(None, "mp"), P("dp", "mp"), P("dp", "mp"), P("dp", "mp"), P())
    return jax.shard_map(
        on_device,
        mesh=mesh,
        in_specs=placed,
        out_specs=(P(None, "mp"), P("dp", "mp"), P("dp", "mp"), P("dp", "mp")),
        check_vma=False,
    )
```
